32 devices in a mesh: dp: 4 (over x, core), vocab: 8 (over z, y).
Axes of the slice: x: 2, y: 2, z: 4, core: 2. Of those that a mesh axis runs over, the one named last changes fastest.
Arguments:
- policy_hidden: bfloat16 [512, 4096], P('dp'), may hold values from -84 to 84
- policy_weight: bfloat16 [4096, 65536], P('dp', 'vocab'), may hold values from -0.09375 to 0.09375
- reference_hidden: bfloat16 [512, 4096], P(('dp', 'vocab')), may hold values from -84 to 84
- reference_weight: bfloat16 [4096, 65536], P(None, ('dp', 'vocab')), may hold values from -0.09375 to 0.09375
- targets: int32 [512], replicated, may hold values from 0 to 65535
- response_mask: int32 [512], replicated, may hold values 0 or 1
- pair_index: int32 [16], replicated, may hold values from 0 to 15, each once
Outputs:
- hidden_grad: bfloat16 [512, 4096], P('vocab', 'dp')
- weight_grad: bfloat16 [4096, 65536], P('dp', 'vocab')
- total_loss: float32 [], replicated
The draws below stay inside these ranges and needn't reach their ends.
Inputs may be any that keep to these rules, and one draw needn't show every extreme that they name: `pair_index`: each number of 0 to 15 once; entries 2p and 2p + 1 are the chosen and the rejected sequence of pair p.
All inputs are finite; a program needn't handle non-finite values.
Results may differ from the reference program's by a relative error of at most 0.005.
The reference program's roundings to bfloat16 on the way (of `logit_grad`) count: a program that leaves them out, or rounds other values in their place, can miss the bound.
Values may be sent and summed in bfloat16 or wider, within the bound.
A program may use at most 128 MiB of HBM per device.

```python
import math
import jax
import jax.numpy as jnp
import numpy as np
from jax import lax

D = 4096
VOCAB = 65536
SEQ_LEN = 32
SEQS = 16
TOKENS = 512


def scaled_rows(key, salt):
    folded = jax.random.fold_in(key, salt)
    key_value = jax.random.fold_in(folded, 1)
    return 3.0 * jnp.clip(jax.random.normal(key_value, (TOKENS, D), jnp.float32), -6.0, 6.0)


def draw_policy_hidden(key, part):
    return scaled_rows(key, 11).astype(jnp.bfloat16)


def draw_reference_hidden(key, part):
    return scaled_rows(key, 23).astype(jnp.bfloat16)


def touch_ends(array, stream_key, smallest, top_value):
    longest = array.shape.index(max(array.shape))
    spots = []
    for shift in (0, 1):
        where = [jax.random.randint(jax.random.fold_in(stream_key, axis), (), 0, length) for axis, length in enumerate(array.shape)]
        where[longest] = (where[longest] + shift) % array.shape[longest]
        spots.append(tuple(where))
    return array.at[spots[0]].set(smallest).at[spots[1]].set(top_value)


def levels(stream_key, shape, cuts, least, high):
    def one(axis_at, parts):
        steps = jax.random.uniform(jax.random.fold_in(jax.random.fold_in(stream_key, 6), axis_at), (parts,), jnp.float32, least / len(cuts), high / len(cuts))
        return jnp.repeat(jnp.exp(steps), shape[axis_at] // parts).reshape((-1,) + (1,) * (len(shape) - axis_at - 1))

    level = one(*cuts[0])
    for cut in cuts[1:]:
        level = level * one(*cut)
    return level


def rank_bounds(amount, skew):
    weights = [(1 << 20) // math.isqrt(standing ** skew) + 1 for standing in range(1, amount + 1)]
    scale = 1 + sum(weights) // (1 << 30)
    return np.cumsum(np.array([max(1, weight // scale) for weight in weights]))


def skewed_ids(stream_key, dims, amount, slope):
    listing = rank_bounds(amount, slope)
    lot = jax.random.randint(jax.random.fold_in(stream_key, 1), dims, 0, int(listing[amount - 1]))
    standing = jnp.searchsorted(jnp.asarray(listing, jnp.int32), lot, side="right")
    return jax.random.permutation(jax.random.fold_in(stream_key, 2), amount)[standing].astype(jnp.int32)


def scatter_about(key, dims, scale, reach, shards=(), kind=jnp.bfloat16):
    array = jax.random.normal(key, dims, jnp.float32) * scale
    if len(shards) > 0:
        array = levels(key, dims, shards, -0.22, 0.18) * array
    return jnp.clip(array, min=-reach, max=reach).astype(kind)


def setup_inputs(seed: int = 0) -> dict:
    key_of = jax.random.split(jax.random.key(seed), 8)
    policy_hidden = draw_policy_hidden(jax.random.fold_in(key_of[7], 71), 0)
    policy_weight = scatter_about(key_of[1], (D, VOCAB), D ** -0.5, 0.09375, ((0, 4), (1, 8)))
    reference_hidden = draw_reference_hidden(jax.random.fold_in(key_of[7], 71), 0)
    reference_weight = scatter_about(key_of[3], (D, VOCAB), D ** -0.5, 0.09375, ((1, 32),))
    targets = touch_ends(skewed_ids(key_of[4], (TOKENS,), VOCAB, 2), jax.random.fold_in(key_of[4], 3), 0, VOCAB - 1).astype(jnp.int32)
    response_mask = touch_ends((jax.random.randint(key_of[5], (TOKENS,), 0, 4) < 3).astype(jnp.int32), jax.random.fold_in(key_of[5], 1), 0, 1)
    pair_index = jax.random.permutation(key_of[6], SEQS).astype(jnp.int32)
    return {"policy_hidden": policy_hidden, "policy_weight": policy_weight, "reference_hidden": reference_hidden, "reference_weight": reference_weight, "targets": targets, "response_mask": response_mask, "pair_index": pair_index}


beta = 0.1
loss_scale = 4096.0
block_size = 64


def pair_terms(log_ratio, pair_index):
    chosen = pair_index[0::2]
    rejected = pair_index[1::2]
    margin = beta * (log_ratio[chosen] - log_ratio[rejected])
    pair_count = chosen.shape[0]
    total_loss = jnp.sum(jax.nn.softplus(-margin)) / pair_count
    weight = -beta * loss_scale * jax.nn.sigmoid(-margin) / pair_count
    numbers = jnp.arange(log_ratio.shape[0], dtype=jnp.int32)[:, None]
    factor = jnp.sum(jnp.where(numbers == chosen[None, :], weight[None, :], 0.0) - jnp.where(numbers == rejected[None, :], weight[None, :], 0.0), axis=1)
    return total_loss, factor


def token_logp(hidden, weight, targets):
    blocks = hidden.shape[0] // block_size

    def block_logp(inputs):
        row_block, target_block = inputs
        logits = jnp.dot(row_block, weight, preferred_element_type=jnp.float32)
        largest = jnp.max(logits, axis=1)
        exp_total = jnp.sum(jnp.exp(logits - largest[:, None]), axis=1)
        picked = jnp.take_along_axis(logits, target_block[:, None], axis=1)[:, 0]
        return picked - largest - jnp.log(exp_total)

    return lax.map(block_logp, (hidden.reshape(blocks, block_size, hidden.shape[1]), targets.reshape(blocks, block_size))).reshape(-1)


def reference(policy_hidden, policy_weight, reference_hidden, reference_weight, targets, response_mask, pair_index):
    policy_logp = token_logp(policy_hidden, policy_weight, targets)
    reference_logp = token_logp(reference_hidden, reference_weight, targets)
    active = response_mask.astype(jnp.float32)
    log_ratio = jnp.sum((active * (policy_logp - reference_logp)).reshape(-1, SEQ_LEN), axis=1)
    total_loss, factor = pair_terms(log_ratio, pair_index)
    token_scale = active * jnp.repeat(factor, SEQ_LEN)
    blocks = policy_hidden.shape[0] // block_size
    vocab_ids = lax.broadcasted_iota(jnp.int32, (block_size, policy_weight.shape[1]), 1)

    def backward(weight_grad, inputs):
        row_block, target_block, scale_block = inputs
        logits = jnp.dot(row_block, policy_weight, preferred_element_type=jnp.float32)
        largest = jnp.max(logits, axis=1, keepdims=True)
        log_total = largest + jnp.log(jnp.sum(jnp.exp(logits - largest), axis=1, keepdims=True))
        onehot = (vocab_ids == target_block[:, None]).astype(jnp.float32)
        logit_grad = (scale_block[:, None] * (onehot - jnp.exp(logits - log_total))).astype(jnp.bfloat16)
        weight_grad = weight_grad + jnp.dot(row_block.T, logit_grad, preferred_element_type=jnp.float32)
        row_grad = jnp.dot(logit_grad, policy_weight.T, preferred_element_type=jnp.float32).astype(jnp.bfloat16)
        return weight_grad, row_grad

    weight_grad, hidden_grad = lax.scan(backward, jnp.zeros(policy_weight.shape, jnp.float32), (policy_hidden.reshape(blocks, block_size, policy_hidden.shape[1]), targets.reshape(blocks, block_size), token_scale.reshape(blocks, block_size)))
    return hidden_grad.reshape(policy_hidden.shape), weight_grad.astype(jnp.bfloat16), total_loss
```

```python
import functools

import jax
import jax.numpy as jnp
from jax import lax
from jax.experimental import pallas as pl
from jax.experimental.pallas import tpu as pltpu
from jax.sharding import PartitionSpec as P

SEQ_LEN = 32
CORES = 2
STEPS = 32767.0

beta = 0.1
loss_scale = 4096.0


def pair_terms(log_ratio, pair_index):
    chosen = pair_index[0::2]
    rejected = pair_index[1::2]
    numbers = jnp.arange(log_ratio.shape[0], dtype=jnp.int32)[:, None]
    is_chosen = numbers == chosen[None, :]
    is_rejected = numbers == rejected[None, :]
    signed = jnp.where(is_chosen, 1.0, 0.0) - jnp.where(is_rejected, 1.0, 0.0)
    margin = beta * jnp.sum(signed * log_ratio[:, None], axis=0)
    pair_count = chosen.shape[0]
    total_loss = jnp.sum(jax.nn.softplus(-margin)) / pair_count
    weight = -beta * loss_scale * jax.nn.sigmoid(-margin) / pair_count
    factor = jnp.sum(signed * weight[None, :], axis=1)
    return (total_loss, factor)


def greet(d, v, data_peers, vocab_peers):
    barrier = pltpu.get_barrier_semaphore()
    for peer in data_peers:
        pl.semaphore_signal(
            barrier, inc=1, device_id=(peer, v), device_id_type=pl.DeviceIdType.MESH
        )
    for peer in vocab_peers:
        pl.semaphore_signal(
            barrier, inc=1, device_id=(d, peer), device_id_type=pl.DeviceIdType.MESH
        )
    pl.semaphore_wait(barrier, len(data_peers) + len(vocab_peers))


def remote(source, target, send_sem, recv_sem, peer):
    return pltpu.make_async_remote_copy(
        src_ref=source,
        dst_ref=target,
        send_sem=send_sem,
        recv_sem=recv_sem,
        device_id=peer,
        device_id_type=pl.DeviceIdType.MESH,
    )


def exchange_bits(nd, nv):
    bits = []
    bit = CORES
    while bit < nd:
        bits.append(("dp", bit))
        bit *= 2
    bit = nv // 2
    while bit >= 1:
        bits.append(("vocab", bit))
        bit //= 2
    bits.append(("dp", 1))
    return bits


def row_order(bits, nd, nv):
    names = []
    bit = nd // 2
    while bit >= 1:
        names.append(("dp", bit))
        bit //= 2
    bit = nv // 2
    while bit >= 1:
        names.append(("vocab", bit))
        bit //= 2
    return [names.index(b) for b in reversed(bits)], len(names)


def flip(index, bit):
    return index + bit * (1 - 2 * ((index // bit) % 2))


def forward_kernel(
    nd, nv, pieces, tile, inside,
    hidden, w, ref_in, wr, policy_wanted, reference_wanted,
    logits, stats, cols,
    wbuf, dsend, drecv, xsend, xrecv, ssend, srecv, refh,
    own_sem, w_sem, wr_sem, a_send, a_recv, d_send, d_recv, x_send, x_recv, s_send, s_recv,
    r_own, r_send, r_recv,
):
    d, v = lax.axis_index("dp"), lax.axis_index("vocab")
    chips = nd // CORES
    chip, core = d // CORES, lax.rem(d, CORES)
    partner = chip * CORES + (1 - core)
    depth = wbuf.shape[1]
    tokens = refh.shape[0]
    away = (chips - 1) * pieces
    bits = exchange_bits(nd, nv) if inside else []
    vocab_peers = [flip(v, bit) for axis, bit in bits if axis == "vocab"]
    greet(d, v, [lax.rem(d + k, nd) for k in range(1, nd)], vocab_peers)

    def columns_of(peer):
        return hidden.at[:, pl.ds(pl.multiple_of(peer * depth, depth), depth)]

    moves = []
    for k in range(1, nd):
        peer = lax.rem(d + k, nd)
        move = remote(
            columns_of(peer), cols.at[d], a_send.at[k - 1], a_recv.at[k - 1], (peer, v)
        )
        move.start()
        moves.append(move)
    own_move = pltpu.make_async_copy(columns_of(d), cols.at[d], own_sem)
    own_move.start()

    place = 0
    if inside:
        for s, (axis, bit) in enumerate(bits):
            place = place + lax.rem((d if axis == "dp" else v) // bit, 2) * (2**s)
        per = tokens // (nd * nv)
        own_rows = refh.at[pl.ds(pl.multiple_of(place * per, per), per)]
        ref_move = pltpu.make_async_copy(ref_in, own_rows, r_own)
    else:
        ref_move = pltpu.make_async_copy(ref_in, refh, r_own)
    ref_move.start()

    def exchange(s):
        axis, bit = bits[s]
        size = per * 2**s
        rows = refh.at[pl.ds(pl.multiple_of((place // 2**s) * size, size), size)]
        peer = (flip(d, bit), v) if axis == "dp" else (d, flip(v, bit))
        return remote(rows, rows, r_send.at[s], r_recv.at[s], peer)

    def load(t):
        j = t // 2
        whose = lax.rem(t, 2) * core + (1 - lax.rem(t, 2)) * (1 - core)
        to = lax.rem(chip + j // pieces + 1, chips)
        at = ((to * CORES + whose) * pieces + lax.rem(j, pieces)) * tile
        return pltpu.make_async_copy(
            w.at[:, pl.ds(pl.multiple_of(at, tile), tile)], wbuf.at[t], w_sem.at[t]
        )

    def load_reference(m):
        return pltpu.make_async_copy(
            wr.at[
                pl.ds(pl.multiple_of(lax.rem(m, nd) * depth, depth), depth),
                pl.ds(pl.multiple_of((m // nd) * tile, tile), tile),
            ],
            wbuf.at[m],
            wr_sem.at[m],
        )

    def run(start, stop, step):
        lax.fori_loop(start, stop, lambda i, carry: (step(i), carry)[1], 0)

    run(0, nd * pieces, lambda t: load(t).start())
    ref_move.wait()
    if inside:
        exchange(0).start()
        exchange(0).wait()
        exchange(1).start()
    own_move.wait()
    for move in moves:
        move.wait()

    def product(t):
        load(t).wait()
        return jnp.dot(
            cols[...].reshape(tokens, depth), wbuf[t], preferred_element_type=jnp.float32
        )

    def to_partner(j):
        return remote(dsend.at[j], drecv.at[j], d_send.at[j], d_recv.at[j], (partner, v))

    def to_chip(j):
        peer = (lax.rem(chip + j // pieces + 1, chips) * CORES + core, v)
        return (
            remote(xsend.at[j], xrecv.at[j], x_send.at[j], x_recv.at[j], peer),
            remote(ssend.at[j], srecv.at[j], s_send.at[j], s_recv.at[j], peer),
        )

    def away_step(j):
        dsend[j] = product(2 * j)
        to_partner(j).start()
        part = product(2 * j + 1)
        to_partner(j).wait_recv()
        part = part + drecv[j]
        largest = jnp.maximum(jnp.max(jnp.abs(part)), 1e-30)
        xsend[j] = jnp.round(part * (STEPS / largest)).astype(jnp.int32).astype(jnp.int16)
        ssend[j] = jnp.full(ssend.shape[1:], 1.0 / STEPS, jnp.float32) * largest
        for copy in to_chip(j):
            copy.start()

    def home_step(n):
        dsend[away + n] = product(2 * (away + n))
        to_partner(away + n).start()
        logits[n] = product(2 * (away + n) + 1)

    first = min(1, away)
    run(0, first, away_step)
    if inside:
        exchange(1).wait()
        exchange(2).start()
    run(first, away, away_step)
    run(0, 2 * away, lambda m: load_reference(m).start())
    if inside:
        exchange(2).wait()
        exchange(3).start()
    run(0, pieces, home_step)
    run(2 * away, nd * pieces, lambda m: load_reference(m).start())
    if inside:
        for s in range(4, len(bits)):
            exchange(s - 1).wait()
            exchange(s).start()
        exchange(len(bits) - 1).wait()

    lanes = lax.broadcasted_iota(jnp.int32, (tokens, 128), 1)
    for half in range(2):
        stats[3 * half] = jnp.full((tokens, 128), -3e38, jnp.float32)
        stats[3 * half + 1] = jnp.zeros((tokens, 128), jnp.float32)
        stats[3 * half + 2] = jnp.zeros((tokens, 128), jnp.float32)

    def add_stats(half, value, wanted, n):
        parts = [value[:, g * 128 : (g + 1) * 128] for g in range(tile // 128)]
        before = stats[3 * half]
        top = functools.reduce(jnp.maximum, parts, before)
        total = stats[3 * half + 1] * jnp.exp(before - top)
        pick = stats[3 * half + 2]
        for g, part in enumerate(parts):
            total = total + jnp.exp(part - top)
            pick = pick + jnp.where(lanes + (n * tile + g * 128) == wanted[...], part, 0.0)
        stats[3 * half] = top
        stats[3 * half + 1] = total
        stats[3 * half + 2] = pick

    def reference_step(n):
        total = None
        for k in range(nd):
            load_reference(n * nd + k).wait()
            part = jnp.dot(
                refh[:, k * depth : (k + 1) * depth],
                wbuf[n * nd + k],
                preferred_element_type=jnp.float32,
            )
            total = part if total is None else total + part
        add_stats(1, total, reference_wanted, n)

    run(0, pieces, reference_step)

    def join_step(n):
        to_partner(away + n).wait_recv()
        total = logits[n] + drecv[away + n]
        for k in range(chips - 1):
            j = k * pieces + n
            for copy in to_chip(j):
                copy.wait_recv()
            total = total + xrecv[j].astype(jnp.int32).astype(jnp.float32) * srecv[j, 0:1, 0:1]
        logits[n] = total
        add_stats(0, total, policy_wanted, n)

    run(0, pieces, join_step)
    run(0, away + pieces, lambda j: to_partner(j).wait_send())

    def sent(j):
        for copy in to_chip(j):
            copy.wait_send()

    run(0, away, sent)


def forward(hidden, weight, reference_hidden, reference_weight, policy_wanted, reference_wanted):
    nd, nv = lax.axis_size("dp"), lax.axis_size("vocab")
    tokens = policy_wanted.shape[0]
    depth, width = weight.shape
    full = reference_weight.shape[0]
    block = width // nd
    tile = min(512, block)
    pieces = block // tile
    inside = reference_hidden.shape[0] < tokens
    away = max((nd // CORES - 1) * pieces, 1)
    hops = max(len(exchange_bits(nd, nv)), 1)
    count = nd * pieces
    half = count // 2
    hbm = pl.BlockSpec(memory_space=pl.ANY)
    vmem = pl.BlockSpec(memory_space=pltpu.VMEM)
    dma = pltpu.SemaphoreType.DMA
    f32, bf16 = jnp.float32, jnp.bfloat16
    return pl.pallas_call(
        functools.partial(forward_kernel, nd, nv, pieces, tile, inside),
        out_shape=[
            jax.ShapeDtypeStruct((pieces, tokens, tile), f32),
            jax.ShapeDtypeStruct((6, tokens, 128), f32),
            jax.ShapeDtypeStruct((nd, tokens // nd, depth), bf16),
        ],
        in_specs=[hbm, hbm, hbm, hbm, vmem, vmem],
        out_specs=[vmem, vmem, vmem],
        scratch_shapes=[
            pltpu.VMEM((count, depth, tile), bf16),
            pltpu.VMEM((half, tokens, tile), f32),
            pltpu.VMEM((half, tokens, tile), f32),
            pltpu.VMEM((away, tokens, tile), jnp.int16),
            pltpu.VMEM((away, tokens, tile), jnp.int16),
            pltpu.VMEM((away, 8, 128), f32),
            pltpu.VMEM((away, 8, 128), f32),
            pltpu.VMEM((tokens, full), bf16),
            dma,
            dma((count,)),
            dma((count,)),
            dma((nd - 1,)),
            dma((nd - 1,)),
            dma((half,)),
            dma((half,)),
            dma((away,)),
            dma((away,)),
            dma((away,)),
            dma((away,)),
            dma,
            dma((hops,)),
            dma((hops,)),
        ],
        compiler_params=pltpu.CompilerParams(
            collective_id=1, has_side_effects=True, vmem_limit_bytes=67043328
        ),
        name="forward",
    )(hidden, weight, reference_hidden, reference_weight, policy_wanted, reference_wanted)


def merge(parts, rows):
    tops = [part[:rows] for part in parts]
    top = functools.reduce(jnp.maximum, tops)
    total = sum(part[rows : 2 * rows] * jnp.exp(t - top) for part, t in zip(parts, tops))
    pick = sum(part[2 * rows : 3 * rows] for part in parts)
    return top, total, pick


def stats_kernel(
    nd, nv, rows, own, total_ref, ratio_ref, near, joined, far, send_d, recv_d, send_v, recv_v
):
    d, v = lax.axis_index("dp"), lax.axis_index("vocab")
    data_peers = [lax.rem(d + k, nd) for k in range(1, nd)]
    vocab_peers = [lax.rem(v + k, nv) for k in range(1, nv)]
    greet(d, v, data_peers, vocab_peers)
    copies = [
        remote(own, near.at[k], send_d.at[k], recv_d.at[k], (p, v))
        for k, p in enumerate(data_peers)
    ]
    for copy in copies:
        copy.start()
    for copy in copies:
        copy.wait()
    for half in range(2):
        span = slice(3 * half * rows, 3 * (half + 1) * rows)
        parts = merge([own[span]] + [near[k, span] for k in range(nd - 1)], rows)
        for k, value in enumerate(parts):
            joined[(3 * half + k) * rows : (3 * half + k + 1) * rows] = value
    copies = [
        remote(joined, far.at[k], send_v.at[k], recv_v.at[k], (d, p))
        for k, p in enumerate(vocab_peers)
    ]
    for copy in copies:
        copy.start()
    for copy in copies:
        copy.wait()
    logps = []
    for half in range(2):
        span = slice(3 * half * rows, 3 * (half + 1) * rows)
        top, total, pick = merge([joined[span]] + [far[k, span] for k in range(nv - 1)], rows)
        total = top + jnp.log(total)
        if half == 0:
            total_ref[...] = total
        logps.append(pick - total)
    ratio_ref[...] = logps[0] - logps[1]


def exchange_stats(stats):
    nd, nv = lax.axis_size("dp"), lax.axis_size("vocab")
    rows = stats.shape[0] // 6
    space = pl.BlockSpec(memory_space=pltpu.VMEM)
    return pl.pallas_call(
        functools.partial(stats_kernel, nd, nv, rows),
        out_shape=[jax.ShapeDtypeStruct((rows, 128), jnp.float32)] * 2,
        in_specs=[space],
        out_specs=[space] * 2,
        scratch_shapes=[
            pltpu.VMEM((nd - 1, 6 * rows, 128), jnp.float32),
            pltpu.VMEM((6 * rows, 128), jnp.float32),
            pltpu.VMEM((nv - 1, 6 * rows, 128), jnp.float32),
            pltpu.SemaphoreType.DMA((nd - 1,)),
            pltpu.SemaphoreType.DMA((nd - 1,)),
            pltpu.SemaphoreType.DMA((nv - 1,)),
            pltpu.SemaphoreType.DMA((nv - 1,)),
        ],
        compiler_params=pltpu.CompilerParams(collective_id=0, has_side_effects=True),
        name="exchange_stats",
    )(stats)


def backward_kernel(
    nd, nv, pieces, tile,
    g, w,
    others, hidden,
    wbuf, total, hsend, hrecv,
    w_sem, n_send, n_recv, x_send, x_recv, f_send, f_recv, h_send, h_recv,
):
    d, v = lax.axis_index("dp"), lax.axis_index("vocab")
    chips = nd // CORES
    chip, core = d // CORES, lax.rem(d, CORES)
    partner = chip * CORES + (1 - core)
    parts, sub = g.shape[1], g.shape[2]
    depth = wbuf.shape[1]
    tokens = nv * parts * sub
    greet(
        d,
        v,
        [lax.rem(d + k, nd) for k in range(1, nd)],
        [lax.rem(v + k, nv) for k in range(1, nv)],
    )

    def run(start, stop, step):
        lax.fori_loop(start, stop, lambda i, carry: (step(i), carry)[1], 0)

    def to_chip(k, n):
        peer = (lax.rem(chip + k, chips) * CORES + core, v)
        i = (k - 1) * parts + n
        return remote(
            g.at[:, n], others.at[2 * k - 1, :, n], x_send.at[i], x_recv.at[i], peer
        )

    def to_partner(k, n):
        i = (k - 1) * parts + n
        return remote(
            others.at[2 * k - 1, :, n],
            others.at[2 * k, :, n],
            f_send.at[i],
            f_recv.at[i],
            (partner, v),
        )

    for n in range(parts):
        for k in range(1, chips):
            to_chip(k, n).start()
    near = remote(g, others.at[0], n_send, n_recv, (partner, v))
    near.start()

    def load(t):
        slot = t // pieces
        whose = lax.rem(slot, 2) * (1 - core) + (1 - lax.rem(slot, 2)) * core
        back = slot // 2
        to = lax.rem(chip - back + chips, chips)
        at = ((to * CORES + whose) * pieces + lax.rem(t, pieces)) * tile
        return pltpu.make_async_copy(
            w.at[:, pl.ds(pl.multiple_of(at, tile), tile)], wbuf.at[t], w_sem.at[t]
        )

    run(0, nd * pieces, lambda t: load(t).start())

    def product(piece, t):
        return lax.dot_general(
            piece, wbuf[t], (((1,), (1,)), ((), ())), preferred_element_type=jnp.float32
        )

    def cut(t):
        at = lax.rem(t, pieces) * tile
        return pl.ds(pl.multiple_of(at, tile), tile)

    total[...] = jnp.zeros_like(total)

    def own_step(t):
        load(t).wait()
        piece = g[:, :, :, cut(t)].reshape(tokens, tile)
        total[...] += product(piece, t).reshape(total.shape)

    def near_step(t):
        load(t).wait()
        piece = others[0, :, :, :, cut(t)].reshape(tokens, tile)
        total[...] += product(piece, t).reshape(total.shape)

    run(0, pieces, own_step)
    near.wait()
    run(pieces, 2 * pieces, near_step)
    run(2 * pieces, nd * pieces, lambda t: load(t).wait())

    def to_vocab(n, k):
        peer = lax.rem(v + k, nv)
        i = n * (nv - 1) + k - 1
        return remote(hsend.at[n, peer], hrecv.at[n, k - 1], h_send.at[i], h_recv.at[i], (d, peer))

    def add_piece(slot, n, t):
        piece = others[slot, :, n, :, cut(t)].reshape(nv * sub, tile)
        return product(piece, t)

    def part_step(n):
        for k in range(1, chips):
            to_chip(k, n).wait_recv()
            to_partner(k, n).start()
        value = total[:, n].reshape(nv * sub, depth)
        for k in range(1, chips):
            for p in range(pieces):
                value = value + add_piece(2 * k - 1, n, 2 * k * pieces + p)
        for k in range(1, chips):
            to_partner(k, n).wait_recv()
            for p in range(pieces):
                value = value + add_piece(2 * k, n, (2 * k + 1) * pieces + p)
        hsend[n] = value.astype(jnp.bfloat16).reshape(nv, sub, depth)
        for k in range(1, nv):
            to_vocab(n, k).start()

    run(0, parts, part_step)

    def sum_step(n):
        value = hsend[n, v].astype(jnp.float32)
        for k in range(1, nv):
            to_vocab(n, k).wait_recv()
            value = value + hrecv[n, k - 1].astype(jnp.float32)
        hidden[n] = value.astype(hidden.dtype)

    run(0, parts, sum_step)

    def sent(n):
        for k in range(1, chips):
            to_chip(k, n).wait_send()
            to_partner(k, n).wait_send()
        for k in range(1, nv):
            to_vocab(n, k).wait_send()

    run(0, parts, sent)


def backward(g, weight):
    nd, nv = lax.axis_size("dp"), lax.axis_size("vocab")
    tokens, block = g.shape
    depth = weight.shape[0]
    tile = min(512, block)
    pieces = block // tile
    group = tokens // nv
    sub = 16 if group % 16 == 0 else group
    parts = group // sub
    moves = max((nd // CORES - 1) * parts, 1)
    dma = pltpu.SemaphoreType.DMA
    vmem = pl.BlockSpec(memory_space=pltpu.VMEM)
    others, hidden = pl.pallas_call(
        functools.partial(backward_kernel, nd, nv, pieces, tile),
        out_shape=[
            jax.ShapeDtypeStruct((nd - 1, nv, parts, sub, block), jnp.bfloat16),
            jax.ShapeDtypeStruct((parts, sub, depth), jnp.bfloat16),
        ],
        in_specs=[vmem, pl.BlockSpec(memory_space=pl.ANY)],
        out_specs=[vmem, vmem],
        scratch_shapes=[
            pltpu.VMEM((nd * pieces, depth, tile), jnp.bfloat16),
            pltpu.VMEM((nv, parts, sub, depth), jnp.float32),
            pltpu.VMEM((parts, nv, sub, depth), jnp.bfloat16),
            pltpu.VMEM((parts, nv - 1, sub, depth), jnp.bfloat16),
            dma((nd * pieces,)),
            dma,
            dma,
            dma((moves,)),
            dma((moves,)),
            dma((moves,)),
            dma((moves,)),
            dma((parts * (nv - 1),)),
            dma((parts * (nv - 1),)),
        ],
        compiler_params=pltpu.CompilerParams(
            collective_id=2, has_side_effects=True, vmem_limit_bytes=67043328
        ),
        name="backward",
    )(g.reshape(nv, parts, sub, block), weight)
    return others.reshape(nd - 1, tokens, block), hidden.reshape(group, depth)


def weight_kernel(steps, at_ref, rows_ref, own_ref, others_ref, out_ref):
    i = pl.program_id(0)

    @pl.when(i < steps)
    def _():
        out_ref[...] = jnp.dot(
            rows_ref[...], own_ref[...], preferred_element_type=jnp.float32
        ).astype(out_ref.dtype)

    @pl.when(i >= steps)
    def _():
        out_ref[...] = jnp.dot(
            rows_ref[...], others_ref[0], preferred_element_type=jnp.float32
        ).astype(out_ref.dtype)


def weight_matmul(rows_t, own, others, slot_columns, width):
    depth, tokens = rows_t.shape
    block = own.shape[1]
    tile = min(1024, block)
    steps = block // tile
    count = others.shape[0] + 1
    at = jnp.concatenate(
        [
            (column // tile).astype(jnp.int32) + jnp.arange(steps, dtype=jnp.int32)
            for column in slot_columns
        ]
    )
    return pl.pallas_call(
        functools.partial(weight_kernel, steps),
        grid_spec=pltpu.PrefetchScalarGridSpec(
            num_scalar_prefetch=1,
            grid=(steps * count,),
            in_specs=[
                pl.BlockSpec((depth, tokens), lambda i, at: (0, 0)),
                pl.BlockSpec((tokens, tile), lambda i, at: (0, jnp.minimum(i, steps - 1))),
                pl.BlockSpec(
                    (1, tokens, tile),
                    lambda i, at: (
                        jnp.maximum(i // steps - 1, 0),
                        0,
                        jnp.where(i < steps, 0, lax.rem(i, steps)),
                    ),
                ),
            ],
            out_specs=pl.BlockSpec((depth, tile), lambda i, at: (0, at[i])),
        ),
        out_shape=jax.ShapeDtypeStruct((depth, width), jnp.bfloat16),
        cost_estimate=pl.CostEstimate(
            flops=2 * depth * tokens * width,
            bytes_accessed=2 * (depth * tokens + tokens * width + depth * width),
            transcendentals=0,
        ),
        name="weight_grad",
    )(at, rows_t, own, others)


def local(
    policy_hidden,
    policy_weight,
    reference_hidden,
    reference_weight,
    targets,
    response_mask,
    pair_index,
):
    d = lax.axis_index("dp")
    v = lax.axis_index("vocab")
    nd = lax.axis_size("dp")
    nv = lax.axis_size("vocab")
    chip, core = d // CORES, d % CORES
    chips = nd // CORES
    tokens = targets.shape[0]
    width = policy_weight.shape[1]
    block = width // nd

    bits = exchange_bits(nd, nv)
    order, count = row_order(bits, nd, nv)
    fold = (2,) * count + (-1,)
    inverse = [order.index(k) for k in range(count)]
    inside = reference_hidden.shape[0] % 16 == 0 and len(bits) >= 4
    reference_targets = targets - (d * nv + v) * reference_weight.shape[1]
    if inside:
        reference_targets = reference_targets.reshape(fold).transpose(*order, count).reshape(-1)
    else:
        reference_hidden = lax.all_gather(reference_hidden, ("dp", "vocab"), axis=0, tiled=True)
    base = v * width + d * block
    own_targets = targets - base

    def lanes(x):
        return jnp.broadcast_to(x[:, None], (tokens, 128))

    logits, stats, rows = forward(
        policy_hidden,
        policy_weight,
        reference_hidden,
        reference_weight,
        lanes(own_targets),
        lanes(reference_targets),
    )
    rows = rows.reshape(tokens, -1)
    packed = []
    for half in range(2):
        tops = stats[3 * half]
        top = jnp.max(tops, axis=1)
        total = jnp.sum(stats[3 * half + 1] * jnp.exp(tops - top[:, None]), axis=1)
        pick = jnp.sum(stats[3 * half + 2], axis=1)
        for stat in (top, total, pick):
            if half == 1 and inside:
                stat = stat.reshape(fold).transpose(*inverse, count).reshape(-1)
            packed.append(stat.reshape(-1, 128))
    totals, ratio = exchange_stats(jnp.concatenate(packed))
    active = response_mask.astype(jnp.float32)
    log_ratio = jnp.sum((active * ratio.reshape(-1)).reshape(-1, SEQ_LEN), axis=1)
    total_loss, factor = pair_terms(log_ratio, pair_index)
    scale = active * jnp.repeat(factor, SEQ_LEN)
    policy_total = totals.reshape(-1)

    logits = jnp.concatenate([logits[n] for n in range(logits.shape[0])], axis=1)
    column_ids = lax.broadcasted_iota(jnp.int32, logits.shape, 1)
    onehot = (column_ids == own_targets[:, None]).astype(jnp.float32)
    grad = (scale[:, None] * (onehot - jnp.exp(logits - policy_total[:, None]))).astype(
        jnp.bfloat16
    )
    others, hidden_grad = backward(grad, policy_weight)
    columns = [d * block, (chip * CORES + 1 - core) * block]
    for k in range(1, chips):
        back = (chip - k + chips) % chips
        columns += [(back * CORES + core) * block, (back * CORES + 1 - core) * block]
    weight_grad = weight_matmul(rows.T, grad, others, columns, width)
    return (hidden_grad, weight_grad, total_loss)


def solution(mesh):
    placed = (
        P("dp", None),
        P("dp", "vocab"),
        P(("dp", "vocab"), None),
        P(None, ("dp", "vocab")),
        P(),
        P(),
        P(),
    )
    return jax.shard_map(
        local,
        mesh=mesh,
        in_specs=placed,
        out_specs=(P("vocab", "dp"), P("dp", "vocab"), P()),
        check_vma=False,
    )
```

```python
import functools

import jax
import jax.numpy as jnp
from jax import lax
from jax.experimental import pallas as pl
from jax.experimental.pallas import tpu as pltpu
from jax.sharding import PartitionSpec as P

SEQ_LEN = 32
CORES = 2
STEPS = 32767.0

beta = 0.1
loss_scale = 4096.0


def greet(d, v, data_peers, vocab_peers):
    barrier = pltpu.get_barrier_semaphore()
    for peer in data_peers:
        pl.semaphore_signal(
            barrier, inc=1, device_id=(peer, v), device_id_type=pl.DeviceIdType.MESH
        )
    for peer in vocab_peers:
        pl.semaphore_signal(
            barrier, inc=1, device_id=(d, peer), device_id_type=pl.DeviceIdType.MESH
        )
    pl.semaphore_wait(barrier, len(data_peers) + len(vocab_peers))


def remote(source, target, send_sem, recv_sem, peer):
    return pltpu.make_async_remote_copy(
        src_ref=source,
        dst_ref=target,
        send_sem=send_sem,
        recv_sem=recv_sem,
        device_id=peer,
        device_id_type=pl.DeviceIdType.MESH,
    )


def exchange_bits(nd, nv):
    bits = []
    bit = CORES
    while bit < nd:
        bits.append(("dp", bit))
        bit *= 2
    bit = nv // 2
    while bit >= 1:
        bits.append(("vocab", bit))
        bit //= 2
    bits.append(("dp", 1))
    return bits


def flip(index, bit):
    return index + bit * (1 - 2 * ((index // bit) % 2))


def merge(parts, rows):
    tops = [part[:rows] for part in parts]
    top = functools.reduce(jnp.maximum, tops)
    total = sum(part[rows : 2 * rows] * jnp.exp(t - top) for part, t in zip(parts, tops))
    pick = sum(part[2 * rows : 3 * rows] for part in parts)
    return top, total, pick


def head_kernel(
    nd, nv, pieces, tile, inside, pairs,
    hidden, w, ref_in, wr, numbers, pair_row,
    g, others, hidden_out, cols, loss,
    wbuf, dsend, drecv, xsend, xrecv, ssend, srecv, refh, logits, stats, marks,
    packed, near_stats, joined, far_stats, total_grad, hsend, hrecv,
    own_sem, w_sem, wr_sem, a_send, a_recv, d_send, d_recv, x_send, x_recv, s_send, s_recv,
    r_own, r_send, r_recv, sd_send, sd_recv, sv_send, sv_recv,
    b_sem, n_send, n_recv, gx_send, gx_recv, f_send, f_recv, h_send, h_recv,
):
    d, v = lax.axis_index("dp"), lax.axis_index("vocab")
    chips = nd // CORES
    chip, core = d // CORES, lax.rem(d, CORES)
    partner = chip * CORES + (1 - core)
    depth = wbuf.shape[1]
    tokens = refh.shape[0]
    away = (chips - 1) * pieces
    parts, sub = g.shape[1], g.shape[2]
    rows = tokens // 128
    bits = exchange_bits(nd, nv) if inside else []
    data_peers = [lax.rem(d + k, nd) for k in range(1, nd)]
    vocab_peers = [lax.rem(v + k, nv) for k in range(1, nv)]
    greet(d, v, data_peers, vocab_peers)

    place = 0
    if inside:
        for s, (axis, bit) in enumerate(bits):
            place = place + lax.rem((d if axis == "dp" else v) // bit, 2) * (2**s)
        per = tokens // (nd * nv)
        own_rows = refh.at[pl.ds(pl.multiple_of(place * per, per), per)]
        ref_move = pltpu.make_async_copy(ref_in, own_rows, r_own)
    else:
        ref_move = pltpu.make_async_copy(ref_in, refh, r_own)
    ref_move.start()

    def exchange(s):
        axis, bit = bits[s]
        size = per * 2**s
        rows = refh.at[pl.ds(pl.multiple_of((place // 2**s) * size, size), size)]
        peer = (flip(d, bit), v) if axis == "dp" else (d, flip(v, bit))
        return remote(ref_in if s == 0 else rows, rows, r_send.at[s], r_recv.at[s], peer)

    if inside:
        exchange(0).start()

    def columns_of(peer):
        return hidden.at[:, pl.ds(pl.multiple_of(peer * depth, depth), depth)]

    moves = []
    for k in range(1, nd):
        peer = lax.rem(d + k, nd)
        move = remote(
            columns_of(peer), cols.at[d], a_send.at[k - 1], a_recv.at[k - 1], (peer, v)
        )
        move.start()
        moves.append(move)
    own_move = pltpu.make_async_copy(columns_of(d), cols.at[d], own_sem)
    own_move.start()

    def load(t):
        j = t // 2
        whose = lax.rem(t, 2) * core + (1 - lax.rem(t, 2)) * (1 - core)
        to = lax.rem(chip + j // pieces + 1, chips)
        at = ((to * CORES + whose) * pieces + lax.rem(j, pieces)) * tile
        return pltpu.make_async_copy(
            w.at[:, pl.ds(pl.multiple_of(at, tile), tile)], wbuf.at[t], w_sem.at[t]
        )

    def load_reference(m):
        return pltpu.make_async_copy(
            wr.at[
                pl.ds(pl.multiple_of(lax.rem(m, nd) * depth, depth), depth),
                pl.ds(pl.multiple_of((m // nd) * tile, tile), tile),
            ],
            wbuf.at[m],
            wr_sem.at[m],
        )

    def run(start, stop, step):
        lax.fori_loop(start, stop, lambda i, carry: (step(i), carry)[1], 0)

    run(0, nd * pieces, lambda t: load(t).start())

    lanes = lax.broadcasted_iota(jnp.int32, (tokens, 128), 1)
    lines = lax.broadcasted_iota(jnp.int32, (tokens, 128), 0)
    named = lines
    if inside:
        named = lax.rem(lines, per)
        for s, (axis, bit) in enumerate(bits):
            step = bit * (nv if axis == "dp" else 1) * per
            named = named + lax.rem(lines // (per * 2**s), 2) * step

    def to_column(at, names):
        total = None
        for k in range(rows):
            row = numbers[at + k : at + k + 1].astype(jnp.float32)
            part = jnp.where(names == lanes + k * 128, row, 0.0)
            total = part if total is None else total + part
        return jnp.sum(total, axis=1, keepdims=True)

    def row_to_column(value):
        total = None
        for k in range(rows):
            part = jnp.where(lines == lanes + k * 128, value[k : k + 1], 0.0)
            total = part if total is None else total + part
        return jnp.sum(total, axis=1, keepdims=True)

    def to_rows(column, names, at):
        for k in range(rows):
            packed[at + k : at + k + 1] = jnp.sum(
                jnp.where(names == lanes + k * 128, column, 0.0), axis=0, keepdims=True
            )

    base = v * (nd * pieces * tile) + d * (pieces * tile)
    reference_base = (d * nv + v) * (pieces * tile)
    wanted = to_column(0, lines).astype(jnp.int32) - base
    marks[0] = jnp.broadcast_to(wanted, (tokens, 128)).reshape(marks.shape[1:])
    wanted = to_column(0, named).astype(jnp.int32) - reference_base
    marks[1] = jnp.broadcast_to(wanted, (tokens, 128)).reshape(marks.shape[1:])
    ref_move.wait()
    if inside:
        exchange(0).wait()
        exchange(1).start()
    own_move.wait()
    for move in moves:
        move.wait()

    def product(t):
        load(t).wait()
        return jnp.dot(
            cols[...].reshape(tokens, depth), wbuf[t], preferred_element_type=jnp.float32
        )

    def to_partner(j):
        source = dsend.at[lax.rem(j, pieces)]
        return remote(source, drecv.at[j], d_send.at[j], d_recv.at[j], (partner, v))

    def send_partner(j):
        @pl.when(j >= pieces)
        def _():
            to_partner(j - pieces).wait_send()

        dsend[lax.rem(j, pieces)] = product(2 * j)
        to_partner(j).start()

    def to_chip(j):
        peer = (lax.rem(chip + j // pieces + 1, chips) * CORES + core, v)
        return (
            remote(xsend.at[j], xrecv.at[j], x_send.at[j], x_recv.at[j], peer),
            remote(ssend.at[j], srecv.at[j], s_send.at[j], s_recv.at[j], peer),
        )

    def away_step(j):
        send_partner(j)
        part = product(2 * j + 1)
        to_partner(j).wait_recv()
        part = part + drecv[j]
        largest = jnp.maximum(jnp.max(jnp.abs(part)), 1e-30)
        xsend[j] = jnp.round(part * (STEPS / largest)).astype(jnp.int32).astype(jnp.int16)
        ssend[j] = jnp.full(ssend.shape[1:], 1.0 / STEPS, jnp.float32) * largest
        for copy in to_chip(j):
            copy.start()

    def home_step(n):
        send_partner(away + n)
        logits[n] = product(2 * (away + n) + 1).reshape(logits.shape[1:])

    late = max(away - 1, 0)
    if inside:
        exchange(1).wait()
        exchange(2).start()
    run(0, late, away_step)
    if inside:
        exchange(2).wait()
        exchange(3).start()
    run(late, away, away_step)
    run(0, 2 * away, lambda m: load_reference(m).start())
    run(0, pieces, home_step)
    run(2 * away, nd * pieces, lambda m: load_reference(m).start())

    for half in range(2):
        stats[3 * half] = jnp.full((tokens, 128), -3e38, jnp.float32)
        stats[3 * half + 1] = jnp.zeros((tokens, 128), jnp.float32)
        stats[3 * half + 2] = jnp.zeros((tokens, 128), jnp.float32)

    def add_stats(half, value, n):
        wanted = marks[half].reshape(tokens, 128)
        cuts = [value[:, i * 128 : (i + 1) * 128] for i in range(tile // 128)]
        before = stats[3 * half]
        top = functools.reduce(jnp.maximum, cuts, before)
        total = stats[3 * half + 1] * jnp.exp(before - top)
        pick = stats[3 * half + 2]
        for i, part in enumerate(cuts):
            total = total + jnp.exp(part - top)
            pick = pick + jnp.where(lanes + (n * tile + i * 128) == wanted, part, 0.0)
        stats[3 * half] = top
        stats[3 * half + 1] = total
        stats[3 * half + 2] = pick

    def join_step(n):
        to_partner(away + n).wait_recv()
        total = logits[n].reshape(tokens, tile) + drecv[away + n]
        for k in range(chips - 1):
            j = k * pieces + n
            for copy in to_chip(j):
                copy.wait_recv()
            total = total + xrecv[j].astype(jnp.int32).astype(jnp.float32) * srecv[j, 0:1, 0:1]
        logits[n] = total.reshape(logits.shape[1:])
        add_stats(0, total, n)

    run(0, pieces // 2, join_step)
    if inside:
        for s in range(4, len(bits)):
            exchange(s - 1).wait()
            exchange(s).start()
    run(pieces // 2, pieces - 1, join_step)
    if inside:
        exchange(len(bits) - 1).wait()

    def reference_step(n):
        total = None
        for k in range(nd):
            load_reference(n * nd + k).wait()
            part = jnp.dot(
                refh[:, k * depth : (k + 1) * depth],
                wbuf[n * nd + k],
                preferred_element_type=jnp.float32,
            )
            total = part if total is None else total + part
        add_stats(1, total, n)

    def pack_stats(half, names):
        tops = stats[3 * half]
        top = jnp.max(tops, axis=1, keepdims=True)
        total = jnp.sum(stats[3 * half + 1] * jnp.exp(tops - top), axis=1, keepdims=True)
        pick = jnp.sum(stats[3 * half + 2], axis=1, keepdims=True)
        for i, column in enumerate((top, total, pick)):
            to_rows(column, names, (3 * half + i) * rows)

    run(0, pieces, reference_step)

    def load_again(t):
        slot = t // pieces
        whose = lax.rem(slot, 2) * (1 - core) + (1 - lax.rem(slot, 2)) * core
        to = lax.rem(chip - slot // 2 + chips, chips)
        at = ((to * CORES + whose) * pieces + lax.rem(t, pieces)) * tile
        return pltpu.make_async_copy(
            w.at[:, pl.ds(pl.multiple_of(at, tile), tile)], wbuf.at[t], b_sem.at[t]
        )

    run(0, nd * pieces, lambda t: load_again(t).start())
    pack_stats(1, named)

    run(pieces - 1, pieces, join_step)
    pack_stats(0, lines)

    copies = [
        remote(packed, near_stats.at[k], sd_send.at[k], sd_recv.at[k], (p, v))
        for k, p in enumerate(data_peers)
    ]
    for copy in copies:
        copy.start()
    for copy in copies:
        copy.wait()
    for half in range(2):
        span = slice(3 * half * rows, 3 * (half + 1) * rows)
        merged = merge([packed[span]] + [near_stats[k, span] for k in range(nd - 1)], rows)
        for i, value in enumerate(merged):
            joined[(3 * half + i) * rows : (3 * half + i + 1) * rows] = value
    copies = [
        remote(joined, far_stats.at[k], sv_send.at[k], sv_recv.at[k], (d, p))
        for k, p in enumerate(vocab_peers)
    ]
    for copy in copies:
        copy.start()
    for copy in copies:
        copy.wait()
    logps = []
    for half in range(2):
        span = slice(3 * half * rows, 3 * (half + 1) * rows)
        top, total, pick = merge([joined[span]] + [far_stats[k, span] for k in range(nv - 1)], rows)
        total = top + jnp.log(total)
        if half == 0:
            policy_total = row_to_column(total)
        logps.append(pick - total)
    ratio = row_to_column(logps[0] - logps[1])

    active = to_column(rows, lines)
    member = jnp.where(lines // SEQ_LEN == pair_row[0:1], active, 0.0)
    log_ratio = jnp.sum(member * ratio, axis=0, keepdims=True)
    log_ratio = jnp.broadcast_to(log_ratio, (8, 128))
    lane = lax.broadcasted_iota(jnp.int32, (8, 128), 1)
    even = lax.rem(lane, 2) == 0
    mate = jnp.where(even, pltpu.roll(log_ratio, 127, 1), pltpu.roll(log_ratio, 1, 1))
    margin = beta * jnp.where(even, log_ratio - mate, mate - log_ratio)
    lost = jnp.maximum(-margin, 0.0) + jnp.log1p(jnp.exp(-jnp.abs(margin)))
    lost = jnp.where(even & (lane < 2 * pairs), lost, 0.0)
    loss[...] = jnp.broadcast_to(jnp.sum(lost, axis=1, keepdims=True) / pairs, (8, 128))
    chance = 1.0 / (1.0 + jnp.exp(jnp.minimum(margin, 80.0)))
    factor = jnp.where(even, -beta, beta) * loss_scale * chance / pairs
    scale = jnp.sum(member * factor[0:1], axis=1, keepdims=True)
    stats[0] = jnp.broadcast_to(policy_total, (tokens, 128))
    stats[1] = jnp.broadcast_to(scale, (tokens, 128))

    def grad_to_chip(k, n):
        peer = (lax.rem(chip + k, chips) * CORES + core, v)
        i = (k - 1) * parts + n
        return remote(g.at[:, n], others.at[2 * k - 1, :, n], gx_send.at[i], gx_recv.at[i], peer)

    def forward_on(k, n):
        i = (k - 1) * parts + n
        return remote(
            others.at[2 * k - 1, :, n],
            others.at[2 * k, :, n],
            f_send.at[i],
            f_recv.at[i],
            (partner, v),
        )

    part_lanes = lax.broadcasted_iota(jnp.int32, (nv, sub, 128), 2)
    by_part = (nv, parts, sub, 128)
    for n in range(parts):
        whole = stats[0].reshape(by_part)[:, n]
        size = stats[1].reshape(by_part)[:, n]
        mark = marks[0, :, n]
        for p in range(pieces):
            for i in range(tile // 128):
                value = jnp.exp(logits[p, :, n, :, i * 128 : (i + 1) * 128] - whole)
                hit = jnp.where(part_lanes + (p * tile + i * 128) == mark, 1.0, 0.0)
                at = p * tile + i * 128
                g[:, n, :, at : at + 128] = (size * (hit - value)).astype(g.dtype)
        for k in range(1, chips):
            grad_to_chip(k, n).start()
    near = remote(g, others.at[0], n_send, n_recv, (partner, v))
    near.start()

    def hidden_product(piece, t):
        return lax.dot_general(
            piece, wbuf[t], (((1,), (1,)), ((), ())), preferred_element_type=jnp.float32
        )

    def cut(t):
        return pl.ds(pl.multiple_of(lax.rem(t, pieces) * tile, tile), tile)

    total_grad[...] = jnp.zeros_like(total_grad)

    def own_step(t):
        load_again(t).wait()
        piece = g[:, :, :, cut(t)].reshape(tokens, tile)
        total_grad[...] += hidden_product(piece, t).reshape(total_grad.shape)

    def near_step(t):
        load_again(t).wait()
        piece = others[0, :, :, :, cut(t)].reshape(tokens, tile)
        total_grad[...] += hidden_product(piece, t).reshape(total_grad.shape)

    run(0, pieces, own_step)
    near.wait()
    run(pieces, 2 * pieces, near_step)
    run(2 * pieces, nd * pieces, lambda t: load_again(t).wait())

    def to_vocab(n, k):
        peer = lax.rem(v + k, nv)
        i = n * (nv - 1) + k - 1
        return remote(hsend.at[n, peer], hrecv.at[n, k - 1], h_send.at[i], h_recv.at[i], (d, peer))

    def add_piece(slot, n, p, t):
        piece = others[slot, :, n, :, p * tile : (p + 1) * tile].reshape(nv * sub, tile)
        return hidden_product(piece, t)

    def part_step(n):
        for k in range(1, chips):
            grad_to_chip(k, n).wait_recv()
            forward_on(k, n).start()
        value = total_grad[:, n].reshape(nv * sub, depth)
        for k in range(1, chips):
            for p in range(pieces):
                value = value + add_piece(2 * k - 1, n, p, 2 * k * pieces + p)
        for k in range(1, chips):
            forward_on(k, n).wait_recv()
            for p in range(pieces):
                value = value + add_piece(2 * k, n, p, (2 * k + 1) * pieces + p)
        hsend[n] = value.astype(jnp.bfloat16).reshape(nv, sub, depth)
        for k in range(1, nv):
            to_vocab(n, k).start()

    run(0, parts, part_step)

    def sum_step(n):
        value = hsend[n, v].astype(jnp.float32)
        for k in range(1, nv):
            to_vocab(n, k).wait_recv()
            value = value + hrecv[n, k - 1].astype(jnp.float32)
        hidden_out[n] = value.astype(hidden_out.dtype)

    run(0, parts, sum_step)

    def part_sent(n):
        for k in range(1, chips):
            grad_to_chip(k, n).wait_send()
            forward_on(k, n).wait_send()
        for k in range(1, nv):
            to_vocab(n, k).wait_send()

    run(0, parts, part_sent)
    run(away, away + pieces, lambda j: to_partner(j).wait_send())

    def sent(j):
        for copy in to_chip(j):
            copy.wait_send()

    run(0, away, sent)


def head(hidden, weight, reference_hidden, reference_weight, targets, mask, pair_index):
    nd, nv = lax.axis_size("dp"), lax.axis_size("vocab")
    tokens = targets.shape[0]
    depth, width = weight.shape
    full = reference_weight.shape[0]
    block = width // nd
    tile = min(512, block)
    pieces = block // tile
    rows = tokens // 128
    group = tokens // nv
    sub = 16 if group % 16 == 0 else group
    parts = group // sub
    inside = reference_hidden.shape[0] < tokens
    away = max((nd // CORES - 1) * pieces, 1)
    hops = max(len(exchange_bits(nd, nv)), 1)
    moves = max((nd // CORES - 1) * parts, 1)
    count = nd * pieces
    half = count // 2
    hbm = pl.BlockSpec(memory_space=pl.ANY)
    vmem = pl.BlockSpec(memory_space=pltpu.VMEM)
    dma = pltpu.SemaphoreType.DMA
    f32, bf16 = jnp.float32, jnp.bfloat16
    numbers = jnp.concatenate([targets, mask]).reshape(2 * rows, 128)
    pairs = pair_index.shape[0] // 2
    pair_row = jnp.pad(pair_index, (0, 128 - 2 * pairs), constant_values=-1)
    pair_row = jnp.broadcast_to(pair_row[None], (8, 128))
    g, others, hidden_grad, cols, loss = pl.pallas_call(
        functools.partial(head_kernel, nd, nv, pieces, tile, inside, pairs),
        out_shape=[
            jax.ShapeDtypeStruct((nv, parts, sub, block), bf16),
            jax.ShapeDtypeStruct((nd - 1, nv, parts, sub, block), bf16),
            jax.ShapeDtypeStruct((parts, sub, depth), bf16),
            jax.ShapeDtypeStruct((nd, tokens // nd, depth), bf16),
            jax.ShapeDtypeStruct((8, 128), f32),
        ],
        in_specs=[hbm, hbm, hbm, hbm, vmem, vmem],
        out_specs=[vmem] * 5,
        scratch_shapes=[
            pltpu.VMEM((count, depth, tile), bf16),
            pltpu.VMEM((pieces, tokens, tile), f32),
            pltpu.VMEM((half, tokens, tile), f32),
            pltpu.VMEM((away, tokens, tile), jnp.int16),
            pltpu.VMEM((away, tokens, tile), jnp.int16),
            pltpu.VMEM((away, 8, 128), f32),
            pltpu.VMEM((away, 8, 128), f32),
            pltpu.VMEM((tokens, full), bf16),
            pltpu.VMEM((pieces, nv, parts, sub, tile), f32),
            pltpu.VMEM((6, tokens, 128), f32),
            pltpu.VMEM((2, nv, parts, sub, 128), jnp.int32),
            pltpu.VMEM((6 * rows, 128), f32),
            pltpu.VMEM((nd - 1, 6 * rows, 128), f32),
            pltpu.VMEM((6 * rows, 128), f32),
            pltpu.VMEM((nv - 1, 6 * rows, 128), f32),
            pltpu.VMEM((nv, parts, sub, depth), f32),
            pltpu.VMEM((parts, nv, sub, depth), bf16),
            pltpu.VMEM((parts, nv - 1, sub, depth), bf16),
            dma,
            dma((count,)),
            dma((count,)),
            dma((nd - 1,)),
            dma((nd - 1,)),
            dma((half,)),
            dma((half,)),
            dma((away,)),
            dma((away,)),
            dma((away,)),
            dma((away,)),
            dma,
            dma((hops,)),
            dma((hops,)),
            dma((nd - 1,)),
            dma((nd - 1,)),
            dma((nv - 1,)),
            dma((nv - 1,)),
            dma((count,)),
            dma,
            dma,
            dma((moves,)),
            dma((moves,)),
            dma((moves,)),
            dma((moves,)),
            dma((parts * (nv - 1),)),
            dma((parts * (nv - 1),)),
        ],
        compiler_params=pltpu.CompilerParams(
            collective_id=0, has_side_effects=True, vmem_limit_bytes=67043328
        ),
        name="head",
    )(hidden, weight, reference_hidden, reference_weight, numbers, pair_row)
    return (
        g.reshape(tokens, block),
        others.reshape(nd - 1, tokens, block),
        hidden_grad.reshape(group, depth),
        cols.reshape(tokens, depth),
        loss[0, 0],
    )


def weight_kernel(steps, at_ref, rows_ref, own_ref, others_ref, out_ref):
    i = pl.program_id(0)

    def product(g):
        return lax.dot_general(
            rows_ref[...], g, (((0,), (0,)), ((), ())), preferred_element_type=jnp.float32
        ).astype(out_ref.dtype)

    @pl.when(i < steps)
    def _():
        out_ref[...] = product(own_ref[...])

    @pl.when(i >= steps)
    def _():
        out_ref[...] = product(others_ref[0])


def weight_matmul(rows, own, others, slot_columns, width):
    tokens, depth = rows.shape
    block = own.shape[1]
    tile = min(1024, block)
    steps = block // tile
    count = others.shape[0] + 1
    at = jnp.concatenate(
        [
            (column // tile).astype(jnp.int32) + jnp.arange(steps, dtype=jnp.int32)
            for column in slot_columns
        ]
    )
    return pl.pallas_call(
        functools.partial(weight_kernel, steps),
        grid_spec=pltpu.PrefetchScalarGridSpec(
            num_scalar_prefetch=1,
            grid=(steps * count,),
            in_specs=[
                pl.BlockSpec((tokens, depth), lambda i, at: (0, 0)),
                pl.BlockSpec((tokens, tile), lambda i, at: (0, jnp.minimum(i, steps - 1))),
                pl.BlockSpec(
                    (1, tokens, tile),
                    lambda i, at: (
                        jnp.maximum(i // steps - 1, 0),
                        0,
                        jnp.where(i < steps, 0, lax.rem(i, steps)),
                    ),
                ),
            ],
            out_specs=pl.BlockSpec((depth, tile), lambda i, at: (0, at[i])),
        ),
        out_shape=jax.ShapeDtypeStruct((depth, width), jnp.bfloat16),
        cost_estimate=pl.CostEstimate(
            flops=2 * depth * tokens * width,
            bytes_accessed=2 * (depth * tokens + tokens * width + depth * width),
            transcendentals=0,
        ),
        name="weight_grad",
    )(at, rows, own, others)


def local(
    policy_hidden,
    policy_weight,
    reference_hidden,
    reference_weight,
    targets,
    response_mask,
    pair_index,
):
    d = lax.axis_index("dp")
    v = lax.axis_index("vocab")
    nd = lax.axis_size("dp")
    nv = lax.axis_size("vocab")
    chip, core = d // CORES, d % CORES
    chips = nd // CORES
    width = policy_weight.shape[1]
    block = width // nd
    if reference_hidden.shape[0] % 16 != 0 or len(exchange_bits(nd, nv)) < 4:
        reference_hidden = lax.all_gather(reference_hidden, ("dp", "vocab"), axis=0, tiled=True)
    grad, others, hidden_grad, rows, total_loss = head(
        policy_hidden,
        policy_weight,
        reference_hidden,
        reference_weight,
        targets,
        response_mask,
        pair_index,
    )
    columns = [d * block, (chip * CORES + 1 - core) * block]
    for k in range(1, chips):
        back = (chip - k + chips) % chips
        columns += [(back * CORES + core) * block, (back * CORES + 1 - core) * block]
    weight_grad = weight_matmul(rows, grad, others, columns, width)
    return (hidden_grad, weight_grad, total_loss)


def solution(mesh):
    placed = (
        P("dp", None),
        P("dp", "vocab"),
        P(("dp", "vocab"), None),
        P(None, ("dp", "vocab")),
        P(),
        P(),
        P(),
    )
    return jax.shard_map(
        local,
        mesh=mesh,
        in_specs=placed,
        out_specs=(P("vocab", "dp"), P("dp", "vocab"), P()),
        check_vma=False,
    )
```
